32 devices in a mesh: dp: 8 (over y, x, core), tensor: 4 (over z).
Axes of the slice: x: 2, y: 2, z: 4, core: 2. Of those that a mesh axis runs over, the one named last changes fastest.
Arguments:
- image: bfloat16 [8, 1024, 1536], P('dp'), may hold values from -6 to 6
- text: bfloat16 [8, 154, 1536], P('dp'), may hold values from -6 to 6
- pooled: bfloat16 [8, 1536], P('dp', 'tensor'), may hold values from -6 to 6
- timestep: int32 [8], P('dp'), may hold values from 0 to 999
- grad_image: bfloat16 [8, 1024, 1536], P('dp'), may hold values from -6 to 6
- grad_text: bfloat16 [8, 154, 1536], P('dp'), may hold values from -6 to 6
- ada_weight: bfloat16 [2, 1536, 9216], P(None, 'tensor', 'dp'), may hold values from -0.15625 to 0.15625
- ada_bias: bfloat16 [2, 9216], replicated, may hold values from -2.390625 to 2.390625
- qkv_weight: bfloat16 [2, 1536, 3, 1536], P(None, 'dp', None, 'tensor'), may hold values from -0.102062073 to 0.102062073
- qv_bias: bfloat16 [2, 2, 1536], P(None, None, 'tensor'), may hold values from -3 to 3
- out_weight: bfloat16 [2, 1536, 1536], P(None, 'tensor', 'dp'), may hold values from -1.25 to 1.25
- out_bias: bfloat16 [2, 1536], replicated, may hold values from -2.390625 to 2.390625
- mlp_in_weight: bfloat16 [2, 1536, 6144], P(None, 'dp', 'tensor'), may hold values from -0.15625 to 0.15625
- mlp_in_bias: bfloat16 [2, 6144], P(None, 'tensor'), may hold values from -3 to 3
- mlp_out_weight: bfloat16 [2, 6144, 1536], P(None, 'tensor', 'dp'), may hold values from -0.078125 to 0.078125
- mlp_out_bias: bfloat16 [2, 1536], replicated, may hold values from -2.390625 to 2.390625
Outputs:
- block_image: bfloat16 [8, 1024, 1536], P('dp')
- block_text: bfloat16 [8, 154, 1536], P('dp')
- image_grad: float32 [8, 1024, 1536], P('dp')
- text_grad: float32 [8, 154, 1536], P('dp')
- pooled_grad: float32 [8, 1536], P('dp', 'tensor')
- ada_weight_grad: float32 [2, 1536, 9216], P(None, 'tensor', 'dp')
- ada_bias_grad: float32 [2, 9216], replicated
- qkv_weight_grad: float32 [2, 1536, 3, 1536], P(None, 'dp', None, 'tensor')
- qv_bias_grad: float32 [2, 2, 1536], P(None, None, 'tensor')
- out_weight_grad: float32 [2, 1536, 1536], P(None, 'tensor', 'dp')
- out_bias_grad: float32 [2, 1536], replicated
- mlp_in_weight_grad: float32 [2, 1536, 6144], P(None, 'dp', 'tensor')
- mlp_in_bias_grad: float32 [2, 6144], P(None, 'tensor')
- mlp_out_weight_grad: float32 [2, 6144, 1536], P(None, 'tensor', 'dp')
- mlp_out_bias_grad: float32 [2, 1536], replicated
The draws below stay inside these ranges and needn't reach their ends.
All inputs are finite; a program needn't handle non-finite values.
Results may differ from the reference program's by a relative error of at most 0.02.
Values may be sent and summed in bfloat16 or wider, within the bound.
A program may use at most 256 MiB of HBM per device.

```python
import math
import jax
import jax.numpy as jnp
from jax import lax

D = 1536
HEADS = 24
HEAD_DIM = 64
FF = 6144
LI = 1024
LT = 154
SEQS = 8


def draw_qkv_weight(key, part):
    shape = (2, D, 3, D)
    base = jnp.clip(jax.random.normal(key, shape, jnp.float32), -4.0, 4.0)
    return (base * D ** (-0.5)).astype(jnp.bfloat16)


def with_ends(values, stream_key, smallest, largest):
    index_at = [jax.random.randint(jax.random.fold_in(stream_key, axis), (), 0, length) for axis, length in enumerate(values.shape)]
    widest = values.shape.index(max(values.shape))
    beside = index_at[:widest] + [(index_at[widest] + 1) % values.shape[widest]] + index_at[widest + 1:]
    return values.at[tuple(index_at)].set(smallest).at[tuple(beside)].set(largest)


def shard_levels(key, dims, split, smallest, largest):
    level = 1.0
    for position, parts in split:
        heights = jax.random.uniform(jax.random.fold_in(jax.random.fold_in(key, 6), position), (parts,), jnp.float32, smallest / len(split), largest / len(split))
        level = level * jnp.repeat(jnp.exp(heights), dims[position] // parts).reshape((-1,) + (1,) * (len(dims) - 1 - position))
    return level


def noise(rng, dims, width, reach, cuts=(), kind=jnp.bfloat16):
    array = jax.random.normal(rng, dims, jnp.float32) * width
    if len(cuts) > 0:
        array = shard_levels(rng, dims, cuts, -0.22, 0.18) * array
    return jnp.clip(array, min=-reach, max=reach).astype(kind)


def setup_inputs(seed: int = 0) -> dict:
    key_of = jax.random.split(jax.random.key(seed), 17)
    return {
        "image": noise(key_of[0], (SEQS, LI, D), 1.0, 6.0, ((0, 8),)),
        "text": noise(key_of[1], (SEQS, LT, D), 1.0, 6.0, ((0, 8),)),
        "pooled": noise(key_of[2], (SEQS, D), 1.0, 6.0, ((0, 8), (1, 4))),
        "timestep": with_ends(jax.random.randint(key_of[3], (SEQS,), 0, 1000), jax.random.fold_in(key_of[3], 1), 0, 999).astype(jnp.int32),
        "grad_image": noise(key_of[4], (SEQS, LI, D), 1.0, 6.0, ((0, 8),)),
        "grad_text": noise(key_of[5], (SEQS, LT, D), 1.0, 6.0, ((0, 8),)),
        "ada_weight": noise(key_of[6], (2, D, 6 * D), D ** -0.5, 0.15625, ((1, 4), (2, 8))),
        "ada_bias": noise(key_of[7], (2, 6 * D), 0.4, 2.390625),
        "qkv_weight": draw_qkv_weight(jax.random.fold_in(key_of[16], 71), 0),
        "qv_bias": noise(key_of[9], (2, 2, D), 0.5, 3.0, ((2, 4),)),
        "out_weight": noise(key_of[10], (2, D, D), (D // 64) ** -0.5, 1.25, ((1, 4), (2, 8))),
        "out_bias": noise(key_of[11], (2, D), 0.4, 2.390625),
        "mlp_in_weight": noise(key_of[12], (2, D, FF), D ** -0.5, 0.15625, ((1, 8), (2, 4))),
        "mlp_in_bias": noise(key_of[13], (2, FF), 0.5, 3.0, ((1, 4),)),
        "mlp_out_weight": noise(key_of[14], (2, FF, D), FF ** -0.5, 0.078125, ((1, 4), (2, 8))),
        "mlp_out_bias": noise(key_of[15], (2, D), 0.4, 2.390625),
    }


@jax.custom_vjp
def low(v):
    return lax.optimization_barrier(v.astype(jnp.bfloat16)).astype(jnp.float32)

@jax.custom_vjp
def low_back(v):
    return v

def low_keep(v):
    return (low(v), None)

def low_pass(kept, grad):
    return (grad,)

def back_keep(v):
    return (v, None)

def back_low(kept, grad):
    return (low(grad),)
low.defvjp(low_keep, low_pass)
low_back.defvjp(back_keep, back_low)

def matmul(left, right):
    return jnp.matmul(left, right, precision=lax.Precision.HIGHEST)

def layer_norm(inputs):
    center = inputs - lax.optimization_barrier(jnp.mean(inputs, axis=-1, keepdims=True))
    spread = lax.optimization_barrier(jnp.mean(center * center, axis=-1, keepdims=True))
    return center * lax.rsqrt(spread + 1e-06)

def time_embed(time_steps, first_col, width_count):
    feature_idx = first_col + jnp.arange(width_count, dtype=jnp.int32)
    half_width = D // 2
    frequency = jnp.exp(-math.log(10000.0) * (feature_idx % half_width).astype(jnp.float32) / half_width)
    phase_arg = time_steps.astype(jnp.float32)[:, None] * frequency[None, :]
    return jnp.where(feature_idx[None, :] < half_width, jnp.cos(phase_arg), jnp.sin(phase_arg))

def forward(image_seq, text_seq, cond_seq, params):
    ada_w, ada_b, qkv_w, qv_b, out_w, out_b, w_in, b_in, w_out, b_out = params
    cond_act = low(jax.nn.silu(cond_seq))
    modulations, queries, key_rows, value_rows = ([], [], [], [])
    for modality_branch, tokens in enumerate((image_seq, text_seq)):
        modul = low_back(matmul(cond_act, ada_w[modality_branch]) + ada_b[modality_branch]).reshape(6, D)
        lowered_input = low(layer_norm(tokens) * (1.0 + modul[1]) + modul[0])
        projected = matmul(lowered_input, qkv_w[modality_branch].reshape(D, 3 * D)).reshape(tokens.shape[0], 3, D)
        queries.append(low(low_back(projected[:, 0] + qv_b[modality_branch, 0])))
        key_rows.append(low(low_back(projected[:, 1])))
        value_rows.append(low(low_back(projected[:, 2] + qv_b[modality_branch, 1])))
        modulations.append(modul)
    joint_q = jnp.concatenate(queries, axis=0).reshape(-1, HEADS, HEAD_DIM)
    joint_k = jnp.concatenate(key_rows, axis=0).reshape(-1, HEADS, HEAD_DIM)
    joint_v = jnp.concatenate(value_rows, axis=0).reshape(-1, HEADS, HEAD_DIM)
    raw_scores = jnp.einsum('qhd,khd->hqk', joint_q, joint_k, precision=lax.Precision.HIGHEST)
    scores = low_back(raw_scores * HEAD_DIM ** (-0.5))
    probs = jax.nn.softmax(scores, axis=-1)
    mixed = jnp.einsum('hqk,khd->qhd', low(probs), joint_v, precision=lax.Precision.HIGHEST)
    mixed = low(low_back(mixed)).reshape(-1, D)
    mixed_parts = (mixed[:LI], mixed[LI:])
    results = []
    for modality_branch, tokens in enumerate((image_seq, text_seq)):
        modul = modulations[modality_branch]
        attn_out = low_back(matmul(mixed_parts[modality_branch], out_w[modality_branch]))
        resid = tokens + modul[2] * (attn_out + out_b[modality_branch])
        low_mid = low(layer_norm(resid) * (1.0 + modul[4]) + modul[3])
        upper = low_back(matmul(low_mid, w_in[modality_branch]) + b_in[modality_branch])
        activation_lowered = low(jax.nn.gelu(upper, approximate=True))
        mlp_out = low_back(matmul(activation_lowered, w_out[modality_branch]))
        results.append(resid + modul[5] * (mlp_out + b_out[modality_branch]))
    return (results[0], results[1])

def reference(image, text, pooled, timestep, grad_image, grad_text, ada_weight, ada_bias, qkv_weight, qv_bias, out_weight, out_bias, mlp_in_weight, mlp_in_bias, mlp_out_weight, mlp_out_bias):
    params = tuple((weight.astype(jnp.float32) for weight in (ada_weight, ada_bias, qkv_weight, qv_bias, out_weight, out_bias, mlp_in_weight, mlp_in_bias, mlp_out_weight, mlp_out_bias)))
    condition = pooled.astype(jnp.float32) + time_embed(timestep, 0, D)

    def per_sequence(running, sequence):
        image_seq, text_seq, cond_seq, cot_image, cot_text = sequence
        results, pullback = jax.vjp(forward, image_seq.astype(jnp.float32), text_seq.astype(jnp.float32), cond_seq, params)
        d_image, d_text, d_cond, d_params = pullback((cot_image.astype(jnp.float32), cot_text.astype(jnp.float32)))
        running = jax.tree.map(lambda left, right: left + right, running, d_params)
        return (running, (results[0].astype(jnp.bfloat16), results[1].astype(jnp.bfloat16), d_image, d_text, d_cond))
    zero_grads = jax.tree.map(jnp.zeros_like, params)
    grads, outputs = lax.scan(per_sequence, zero_grads, (image, text, condition, grad_image, grad_text))
    block_image, block_text, image_grad, text_grad, pooled_grad = outputs
    return (block_image, block_text, image_grad, text_grad, pooled_grad, grads[0], grads[1], grads[2], grads[3], grads[4], grads[5], grads[6], grads[7], grads[8], grads[9])
```

```python
import functools
import math

import jax
import jax.numpy as jnp
from jax import lax
from jax.experimental import pallas as pl
from jax.experimental.pallas import tpu as pltpu
from jax.sharding import PartitionSpec as P

D = 1536
HEAD_DIM = 64


MESH = pl.DeviceIdType.MESH
ROWS = 1184


def ar_kernel(n, R, x_ref, o_ref, rin, rx, pb, s1, s2, r1, r2, r3):
    NC = ROWS // R
    me = lax.axis_index("tensor")
    half = n // 2
    left = me < half
    is_mid = (me == half - 1) | (me == half)
    inward = jnp.where(left, me + 1, me - 1)
    outward = jnp.where(left, me - 1, me + 1)
    bar = pltpu.get_barrier_semaphore()
    pl.semaphore_signal(bar, inc=1, device_id={"tensor": inward}, device_id_type=MESH)

    @pl.when(is_mid)
    def _():
        pl.semaphore_signal(bar, inc=1, device_id={"tensor": outward}, device_id_type=MESH)
        pl.semaphore_wait(bar, 2)

    @pl.when(jnp.logical_not(is_mid))
    def _():
        pl.semaphore_wait(bar, 1)

    def sl(k):
        return pl.ds(pl.multiple_of(k * R, R), R)

    def to_mid(k):
        return pltpu.make_async_remote_copy(x_ref.at[sl(k)], rin.at[sl(k)], s1.at[k], r1.at[k],
                                            device_id={"tensor": inward}, device_id_type=MESH)
    def xchg(k):
        return pltpu.make_async_remote_copy(pb.at[sl(k)], rx.at[sl(k)], s1.at[k], r2.at[k],
                                            device_id={"tensor": inward}, device_id_type=MESH)
    def out(k):
        return pltpu.make_async_remote_copy(o_ref.at[sl(k)], o_ref.at[sl(k)], s2.at[k], r3.at[k],
                                            device_id={"tensor": outward}, device_id_type=MESH)

    @pl.when(jnp.logical_not(is_mid))
    def _():
        def send(k, c):
            to_mid(k).start()
            return c
        lax.fori_loop(0, NC, send, 0)
        def fin(k, c):
            out(k).wait_recv()
            to_mid(k).wait_send()
            return c
        lax.fori_loop(0, NC, fin, 0)

    @pl.when(is_mid)
    def _():
        def a(k):
            to_mid(k).wait_recv()
            pb[sl(k)] = (x_ref[sl(k)].astype(jnp.float32) + rin[sl(k)].astype(jnp.float32)).astype(jnp.bfloat16)
            xchg(k).start()
        def b(k):
            xchg(k).wait_recv()
            o_ref[sl(k)] = (pb[sl(k)].astype(jnp.float32) + rx[sl(k)].astype(jnp.float32)).astype(jnp.bfloat16)
            out(k).start()
        L = 2
        for k in range(L):
            a(k)
        def st(k, c):
            a(k)
            b(k - L)
            return c
        lax.fori_loop(L, NC, st, 0)
        for k in range(NC - L, NC):
            b(k)
        def fin(k, c):
            xchg(k).wait_send()
            out(k).wait_send()
            return c
        lax.fori_loop(0, NC, fin, 0)

def ar(x, n, R, cid):
    NC = ROWS // R
    V = lambda: pltpu.VMEM((ROWS, D), jnp.bfloat16)
    S = lambda: pltpu.SemaphoreType.DMA((NC,))
    return pl.pallas_call(
        functools.partial(ar_kernel, n, R),
        out_shape=jax.ShapeDtypeStruct((ROWS, D), jnp.bfloat16),
        in_specs=[pl.BlockSpec(memory_space=pltpu.VMEM)],
        out_specs=pl.BlockSpec(memory_space=pltpu.VMEM),
        scratch_shapes=[V(), V(), V(), S(), S(), S(), S(), S()],
        compiler_params=pltpu.CompilerParams(collective_id=cid, has_side_effects=True, vmem_limit_bytes=60 << 20),
    )(x)

def z_sum(image_part, text_part, size, cid):
    li, lt = image_part.shape[1], text_part.shape[1]
    joint = jnp.concatenate(
        [image_part[0], text_part[0], jnp.zeros((ROWS - li - lt, D), jnp.float32)]
    ).astype(jnp.bfloat16)
    total = ar(joint, size, 32, cid)
    return (
        total[None, :li].astype(jnp.float32),
        total[None, li : li + lt].astype(jnp.float32),
    )


def layer_norm(inputs):
    center = inputs - jnp.mean(inputs, axis=-1, keepdims=True)
    spread = jnp.mean(center * center, axis=-1, keepdims=True)
    return center * lax.rsqrt(spread + 1e-06)


def modulate(inputs, shift_by, scale_by):
    return layer_norm(inputs) * (1.0 + scale_by) + shift_by


def gelu_tanh(inputs):
    return jax.nn.gelu(inputs, approximate=True)


def time_embed(time_steps, first_col, width_count):
    feature_idx = first_col + jnp.arange(width_count, dtype=jnp.int32)
    half_width = D // 2
    frequency = jnp.exp(
        -math.log(10000.0) * (feature_idx % half_width).astype(jnp.float32) / half_width
    )
    phase_arg = time_steps.astype(jnp.float32)[:, None] * frequency[None, :]
    return jnp.where(feature_idx[None, :] < half_width, jnp.cos(phase_arg), jnp.sin(phase_arg))


def split_heads(inputs):
    return inputs.reshape(inputs.shape[0], inputs.shape[1] // HEAD_DIM, HEAD_DIM)


def attend_block(queries, key_rows, value_rows):
    q_heads = split_heads(queries)
    k_heads = split_heads(key_rows)
    v_heads = split_heads(value_rows)
    scores = jnp.einsum(
        "qhd,khd->hqk", q_heads, k_heads, preferred_element_type=jnp.float32
    ) * HEAD_DIM ** (-0.5)
    row_max = jnp.max(scores, axis=-1, keepdims=True)
    exp_scores = jnp.exp(scores - row_max)
    row_sum = jnp.sum(exp_scores, axis=-1, keepdims=True)
    weights = (exp_scores / row_sum).astype(jnp.bfloat16)
    mixed_out = jnp.einsum("hqk,khd->qhd", weights, v_heads, preferred_element_type=jnp.float32)
    logsum = (row_max + jnp.log(row_sum))[..., 0]
    return (mixed_out.reshape(queries.shape).astype(jnp.bfloat16), logsum)


def attend_sequence(sequence):
    queries, key_rows, value_rows = sequence
    half_rows = queries.shape[0] // 2
    blocks = queries.reshape(2, half_rows, queries.shape[1])
    mixed_out, logsum = lax.map(
        lambda block_in: attend_block(block_in, key_rows, value_rows), blocks
    )
    return (mixed_out.reshape(queries.shape), logsum)


def attend_block_back(queries, key_rows, value_rows, grad_rows, logsum):
    q_heads = split_heads(queries)
    k_heads = split_heads(key_rows)
    v_heads = split_heads(value_rows)
    g_heads = split_heads(grad_rows)
    scale_by = HEAD_DIM ** (-0.5)
    scores = (
        jnp.einsum("qhd,khd->hqk", q_heads, k_heads, preferred_element_type=jnp.float32) * scale_by
    )
    prob_rows = jnp.exp(scores - logsum[..., None])
    grad_prob = jnp.einsum("qhd,khd->hqk", g_heads, v_heads, preferred_element_type=jnp.float32)
    row_delta = jnp.sum(grad_prob * prob_rows, axis=-1, keepdims=True)
    grad_score = (prob_rows * (grad_prob - row_delta)).astype(jnp.bfloat16)
    grad_query = (
        jnp.einsum("hqk,khd->qhd", grad_score, k_heads, preferred_element_type=jnp.float32)
        * scale_by
    )
    grad_key = (
        jnp.einsum("hqk,qhd->khd", grad_score, q_heads, preferred_element_type=jnp.float32)
        * scale_by
    )
    grad_value = jnp.einsum(
        "hqk,qhd->khd", prob_rows.astype(jnp.bfloat16), g_heads, preferred_element_type=jnp.float32
    )
    return (
        grad_query.reshape(queries.shape),
        grad_key.reshape(key_rows.shape),
        grad_value.reshape(value_rows.shape),
    )


def attend_sequence_back(sequence):
    queries, key_rows, value_rows, grad_rows, logsum = sequence
    half_rows = queries.shape[0] // 2
    query_blocks = queries.reshape(2, half_rows, queries.shape[1])
    grad_blocks = grad_rows.reshape(2, half_rows, grad_rows.shape[1])

    def block_step(running, block_in):
        query_part, grad_part, logsum_part = block_in
        grad_query, grad_key, grad_value = attend_block_back(
            query_part, key_rows, value_rows, grad_part, logsum_part
        )
        return ((running[0] + grad_key, running[1] + grad_value), grad_query)

    zero_rows = jnp.zeros(key_rows.shape, jnp.float32)
    (grad_key, grad_value), grad_query = lax.scan(
        block_step, (zero_rows, zero_rows), (query_blocks, grad_blocks, logsum)
    )
    return (
        grad_query.reshape(queries.shape).astype(jnp.bfloat16),
        grad_key.astype(jnp.bfloat16),
        grad_value.astype(jnp.bfloat16),
    )


def shards(
    image,
    text,
    pooled,
    timestep,
    grad_image,
    grad_text,
    ada_weight,
    ada_bias,
    qkv_weight,
    qv_bias,
    out_weight,
    out_bias,
    mlp_in_weight,
    mlp_in_bias,
    mlp_out_weight,
    mlp_out_bias,
):
    width_local = pooled.shape[1]
    first_col = lax.axis_index("tensor") * width_local
    condition = pooled.astype(jnp.float32) + time_embed(timestep, first_col, width_local)
    cond_act, silu_pull = jax.vjp(jax.nn.silu, condition)
    cond_low = cond_act.astype(jnp.bfloat16)
    size = lax.axis_size("tensor")
    cond_all = lax.all_gather(cond_low, "dp", axis=0, tiled=True)
    query_key_value_whole, out_full = (
        lax.all_gather(qkv_weight, "dp", axis=1, tiled=True),
        lax.all_gather(out_weight, "dp", axis=2, tiled=True),
    )
    mod_part = jnp.einsum("sc,nce->nse", cond_all, ada_weight, preferred_element_type=jnp.float32)
    mod_part = lax.all_to_all(mod_part, "dp", split_axis=1, concat_axis=2, tiled=True)
    modul = lax.psum(mod_part, "tensor") + ada_bias.astype(jnp.float32)[:, None, :]
    seq_count = modul.shape[1]
    modul = modul.reshape(2, seq_count, 6, 1, D)
    out_bias_f = out_bias.astype(jnp.float32)
    in_bias_f = mlp_in_bias.astype(jnp.float32)
    last_bias_f = mlp_out_bias.astype(jnp.float32)
    pair_bias = qv_bias.astype(jnp.float32)
    streams = (image.astype(jnp.float32), text.astype(jnp.float32))
    cotangents = (grad_image.astype(jnp.float32), grad_text.astype(jnp.float32))
    first_pulls, lowered_input_list, query_list, key_list, value_list = ([], [], [], [], [])
    for modality_branch in range(2):
        normed, first_pull = jax.vjp(
            modulate,
            streams[modality_branch],
            modul[modality_branch, :, 0],
            modul[modality_branch, :, 1],
        )
        lowered_input = normed.astype(jnp.bfloat16)
        projected = jnp.einsum(
            "hbr,rfu->hbfu",
            lowered_input,
            query_key_value_whole[modality_branch],
            preferred_element_type=jnp.float32,
        )
        query_list.append((projected[:, :, 0] + pair_bias[modality_branch, 0]).astype(jnp.bfloat16))
        key_list.append(projected[:, :, 1].astype(jnp.bfloat16))
        value_list.append((projected[:, :, 2] + pair_bias[modality_branch, 1]).astype(jnp.bfloat16))
        first_pulls.append(first_pull)
        lowered_input_list.append(lowered_input)
    joint_q = jnp.concatenate(query_list, axis=1)
    joint_k = jnp.concatenate(key_list, axis=1)
    joint_v = jnp.concatenate(value_list, axis=1)
    attn_mix, logsum = lax.map(attend_sequence, (joint_q, joint_k, joint_v))
    split_at = image.shape[1]
    mix_parts = (attn_mix[:, :split_at], attn_mix[:, split_at:])
    attn_terms = tuple(
        (
            jnp.einsum(
                "acn,nz->acz",
                mix_parts[modality_branch],
                out_full[modality_branch],
                preferred_element_type=jnp.float32,
            )
            for modality_branch in range(2)
        )
    )
    input_weight_whole, output_weight_whole = (
        lax.all_gather(mlp_in_weight, "dp", axis=1, tiled=True),
        lax.all_gather(mlp_out_weight, "dp", axis=2, tiled=True),
    )
    branches, resids, second_pulls, lowered_middle_list = ([], [], [], [])
    attn_terms = tuple(attn_terms)
    attn_sum = z_sum(attn_terms[0], attn_terms[1], size, 1)
    for modality_branch in range(2):
        branch = attn_sum[modality_branch] + out_bias_f[modality_branch]
        resid = streams[modality_branch] + modul[modality_branch, :, 2] * branch
        normed_mid, second_pull = jax.vjp(
            modulate, resid, modul[modality_branch, :, 3], modul[modality_branch, :, 4]
        )
        lowered_middle_list.append(normed_mid.astype(jnp.bfloat16))
        branches.append(branch)
        resids.append(resid)
        second_pulls.append(second_pull)
    gelu_pulls, activation_lowered_list, mlp_terms = ([], [], [])
    for modality_branch in range(2):
        upper = (
            jnp.einsum(
                "wic,ch->wih",
                lowered_middle_list[modality_branch],
                input_weight_whole[modality_branch],
                preferred_element_type=jnp.float32,
            )
            + in_bias_f[modality_branch]
        )
        act_value, gelu_pull = jax.vjp(gelu_tanh, upper)
        activation_lowered = act_value.astype(jnp.bfloat16)
        mlp_terms.append(
            jnp.einsum(
                "qjt,tx->qjx",
                activation_lowered,
                output_weight_whole[modality_branch],
                preferred_element_type=jnp.float32,
            )
        )
        gelu_pulls.append(gelu_pull)
        activation_lowered_list.append(activation_lowered)
    mlp_sum = z_sum(mlp_terms[0], mlp_terms[1], size, 2)
    block_out, gate2_grads = ([], [])
    for modality_branch in range(2):
        second_branch = mlp_sum[modality_branch] + last_bias_f[modality_branch]
        block_out.append(
            (resids[modality_branch] + modul[modality_branch, :, 5] * second_branch).astype(
                jnp.bfloat16
            )
        )
        gate2_grads.append(jnp.sum(cotangents[modality_branch] * second_branch, axis=1))
    bias2_grads, w_out_grads, bias1_grads, w_in_grads, mid_terms = ([], [], [], [], [])
    for modality_branch in range(2):
        cot_rows = cotangents[modality_branch]
        d_mlp = modul[modality_branch, :, 5] * cot_rows
        bias2_grads.append(jnp.sum(d_mlp, axis=(0, 1)))
        mlp_gradient_lowered = d_mlp.astype(jnp.bfloat16)
        w_out_grads.append(
            jnp.einsum(
                "equ,eqo->ou",
                activation_lowered_list[modality_branch],
                mlp_gradient_lowered,
                preferred_element_type=jnp.float32,
            )
        )
        d_act = jnp.einsum(
            "kbp,gp->kbg",
            mlp_gradient_lowered,
            output_weight_whole[modality_branch],
            preferred_element_type=jnp.float32,
        )
        (d_upper,) = gelu_pulls[modality_branch](d_act)
        upper_gradient_lowered = d_upper.astype(jnp.bfloat16)
        bias1_grads.append(jnp.sum(upper_gradient_lowered.astype(jnp.float32), axis=(0, 1)))
        w_in_grads.append(
            jnp.einsum(
                "typ,tyq->pq",
                lowered_middle_list[modality_branch],
                upper_gradient_lowered,
                preferred_element_type=jnp.float32,
            )
        )
        mid_terms.append(
            jnp.einsum(
                "viq,pq->vip",
                upper_gradient_lowered,
                input_weight_whole[modality_branch],
                preferred_element_type=jnp.float32,
            )
        )
    w_in_grad_all = jnp.stack(w_in_grads)
    w_out_grad_all = jnp.stack(w_out_grads)
    w_in_shard, w_out_shard = (
        lax.psum_scatter(
            w_in_grad_all.astype(jnp.bfloat16), "dp", scatter_dimension=1, tiled=True
        ).astype(jnp.float32),
        jnp.swapaxes(
            lax.psum_scatter(
                w_out_grad_all.astype(jnp.bfloat16), "dp", scatter_dimension=1, tiled=True
            ).astype(jnp.float32),
            1,
            2,
        ),
    )
    d_resids, shift2_grads, scale2_grads, gate1_grads, outb_grads = ([], [], [], [], [])
    d_mid = z_sum(mid_terms[0], mid_terms[1], size, 3)
    d_attn_lows = []
    for modality_branch in range(2):
        d_resid, shift_two, scale_two = second_pulls[modality_branch](d_mid[modality_branch])
        d_resid = d_resid + cotangents[modality_branch]
        d_attn = modul[modality_branch, :, 2] * d_resid
        outb_grads.append(jnp.sum(d_attn, axis=(0, 1)))
        gate1_grads.append(jnp.sum(d_resid * branches[modality_branch], axis=1))
        d_attn_lows.append(d_attn.astype(jnp.bfloat16))
        d_resids.append(d_resid)
        shift2_grads.append(shift_two[:, 0])
        scale2_grads.append(scale_two[:, 0])
    out_grads, d_mix_list = ([], [])
    for modality_branch in range(2):
        out_grads.append(
            jnp.einsum(
                "kyb,kyt->tb",
                mix_parts[modality_branch],
                d_attn_lows[modality_branch],
                preferred_element_type=jnp.float32,
            )
        )
        d_mix_list.append(
            jnp.einsum(
                "xkm,am->xka",
                d_attn_lows[modality_branch],
                out_full[modality_branch],
                preferred_element_type=jnp.float32,
            ).astype(jnp.bfloat16)
        )
    d_mix_joint = jnp.concatenate(d_mix_list, axis=1)
    d_query, d_key, d_value = lax.map(
        attend_sequence_back, (joint_q, joint_k, joint_v, d_mix_joint, logsum)
    )
    qkv_grads, pair_grads, in_terms = ([], [], [])
    for modality_branch in range(2):
        rows_from = 0 if modality_branch == 0 else split_at
        rows_to = split_at if modality_branch == 0 else d_query.shape[1]
        projection_gradient = jnp.stack(
            [
                d_query[:, rows_from:rows_to],
                d_key[:, rows_from:rows_to],
                d_value[:, rows_from:rows_to],
            ],
            axis=2,
        )
        qkv_grads.append(
            jnp.einsum(
                "pjw,pjmb->wmb",
                lowered_input_list[modality_branch],
                projection_gradient,
                preferred_element_type=jnp.float32,
            )
        )
        pair_grads.append(
            jnp.stack(
                [
                    jnp.sum(projection_gradient[:, :, 0].astype(jnp.float32), axis=(0, 1)),
                    jnp.sum(projection_gradient[:, :, 2].astype(jnp.float32), axis=(0, 1)),
                ]
            )
        )
        in_terms.append(
            jnp.einsum(
                "rawn,uwn->rau",
                projection_gradient,
                query_key_value_whole[modality_branch],
                preferred_element_type=jnp.float32,
            )
        )
    d_in = z_sum(in_terms[0], in_terms[1], size, 4)
    token_grads, d_mods = ([], [])
    for modality_branch in range(2):
        d_tokens, shift_one, scale_one = first_pulls[modality_branch](d_in[modality_branch])
        token_grads.append(d_tokens + d_resids[modality_branch])
        d_mods.append(
            jnp.stack(
                [
                    shift_one[:, 0],
                    scale_one[:, 0],
                    gate1_grads[modality_branch],
                    shift2_grads[modality_branch],
                    scale2_grads[modality_branch],
                    gate2_grads[modality_branch],
                ],
                axis=1,
            )
        )
    small = [
        jnp.concatenate([d_mods[0].reshape(-1), d_mods[1].reshape(-1)]),
        jnp.stack(pair_grads).reshape(-1),
        jnp.stack(outb_grads).reshape(-1),
        jnp.stack(bias1_grads).reshape(-1),
        jnp.stack(bias2_grads).reshape(-1),
    ]
    every = lax.all_gather(jnp.concatenate(small).astype(jnp.bfloat16), "dp")
    summed = jnp.sum(every.astype(jnp.float32), axis=0)
    at = [0]
    for part in small:
        at.append(at[-1] + part.shape[0])
    adab_sum = summed[: at[1]].reshape(2, 6 * D)
    pair_sum = summed[at[1] : at[2]].reshape(2, 2, -1)
    outb_sum = summed[at[2] : at[3]].reshape(2, -1)
    bias1_sum = summed[at[3] : at[4]].reshape(2, -1)
    bias2_sum = summed[at[4] :].reshape(2, -1)
    cols = ada_weight.shape[2]
    d_mod_cols = lax.dynamic_slice_in_dim(
        every[:, : at[1]].reshape(-1, 2, 6 * D), lax.axis_index("dp") * cols, cols, axis=2
    )
    ada_shard = jnp.einsum(
        "sc,sne->nce", cond_all, d_mod_cols, preferred_element_type=jnp.float32
    )
    d_cond_act = lax.psum_scatter(
        jnp.einsum("sne,nce->sc", d_mod_cols, ada_weight, preferred_element_type=jnp.float32),
        "dp",
        scatter_dimension=0,
        tiled=True,
    )
    (pooled_grad,) = silu_pull(d_cond_act)
    qkv_grad_all = jnp.stack(qkv_grads)
    out_grad_all = jnp.stack(out_grads)
    qkv_shard, out_shard = (
        lax.psum_scatter(
            qkv_grad_all.astype(jnp.bfloat16), "dp", scatter_dimension=1, tiled=True
        ).astype(jnp.float32),
        jnp.swapaxes(
            lax.psum_scatter(
                out_grad_all.astype(jnp.bfloat16), "dp", scatter_dimension=1, tiled=True
            ).astype(jnp.float32),
            1,
            2,
        ),
    )
    return (
        block_out[0],
        block_out[1],
        token_grads[0],
        token_grads[1],
        pooled_grad,
        ada_shard,
        adab_sum,
        qkv_shard,
        pair_sum,
        out_shard,
        outb_sum,
        w_in_shard,
        bias1_sum,
        w_out_shard,
        bias2_sum,
    )


def solution(mesh):
    return jax.shard_map(
        shards,
        mesh=mesh,
        in_specs=(
            P("dp", None, None),
            P("dp", None, None),
            P("dp", "tensor"),
            P("dp"),
            P("dp", None, None),
            P("dp", None, None),
            P(None, "tensor", "dp"),
            P(),
            P(None, "dp", None, "tensor"),
            P(None, None, "tensor"),
            P(None, "tensor", "dp"),
            P(),
            P(None, "dp", "tensor"),
            P(None, "tensor"),
            P(None, "tensor", "dp"),
            P(),
        ),
        out_specs=(
            P("dp", None, None),
            P("dp", None, None),
            P("dp", None, None),
            P("dp", None, None),
            P("dp", "tensor"),
            P(None, "tensor", "dp"),
            P(),
            P(None, "dp", None, "tensor"),
            P(None, None, "tensor"),
            P(None, "tensor", "dp"),
            P(),
            P(None, "dp", "tensor"),
            P(None, "tensor"),
            P(None, "tensor", "dp"),
            P(),
        ),
        check_vma=False,
    )
```

```python
import functools
import math

import jax
import jax.numpy as jnp
from jax import lax
from jax.experimental import pallas as pl
from jax.experimental.pallas import tpu as pltpu
from jax.sharding import PartitionSpec as P

D = 1536
HEAD_DIM = 64
PAIR = 2 * HEAD_DIM
SUB = 64
F32, BF16 = jnp.float32, jnp.bfloat16
NN = (((1,), (0,)), ((), ()))
NT = (((1,), (1,)), ((), ()))
MESH = pl.DeviceIdType.MESH
ANY = pl.BlockSpec(memory_space=pl.ANY)
VM = pl.BlockSpec(memory_space=pltpu.VMEM)
VMEM_MAX = 67_043_328
DMA = pltpu.SemaphoreType.DMA


def dot(left, right, dims=NN):
    return lax.dot_general(left, right, dims, preferred_element_type=F32)


def time_embed(time_steps, first_col, width_count):
    feature_idx = first_col + jnp.arange(width_count, dtype=jnp.int32)
    half_width = D // 2
    frequency = jnp.exp(
        -math.log(10000.0) * (feature_idx % half_width).astype(jnp.float32) / half_width
    )
    phase_arg = time_steps.astype(jnp.float32)[:, None] * frequency[None, :]
    return jnp.where(feature_idx[None, :] < half_width, jnp.cos(phase_arg), jnp.sin(phase_arg))


def norm_rows(rows):
    center = rows - jnp.mean(rows, axis=-1, keepdims=True)
    rstd = lax.rsqrt(jnp.mean(center * center, axis=-1, keepdims=True) + 1e-06)
    return center * rstd, rstd


def start_of(k, li):
    image_pieces = li // SUB
    if isinstance(k, int):
        if k < image_pieces:
            return k * SUB, SUB
        return li + (k - image_pieces) * 80, 80
    return pl.multiple_of(k * SUB, SUB), SUB


class ZSum:
    def __init__(self, size, li, own, come, total, sems):
        self.li, self.own, self.come, self.total = li, own, come, total
        self.s1, self.s2, self.r1, self.r2, self.r3 = sems
        me = lax.axis_index("tensor")
        half = size // 2
        self.mid = (me == half - 1) | (me == half)
        self.end = jnp.logical_not(self.mid)
        self.inward = jnp.where(me < half, me + 1, me - 1)
        self.outward = jnp.where(me < half, me - 1, me + 1)

    def barrier(self):
        bar = pltpu.get_barrier_semaphore()
        pl.semaphore_signal(bar, inc=1, device_id={"tensor": self.inward}, device_id_type=MESH)

        @pl.when(self.mid)
        def _():
            pl.semaphore_signal(bar, inc=1, device_id={"tensor": self.outward}, device_id_type=MESH)
            pl.semaphore_wait(bar, 2)

        @pl.when(self.end)
        def _():
            pl.semaphore_wait(bar, 1)

    def at(self, k):
        r0, n = start_of(k, self.li)
        return pl.ds(r0, n)

    def _copy(self, src, dst, send, recv, k, where):
        return pltpu.make_async_remote_copy(
            src.at[self.at(k)], dst.at[self.at(k)], send.at[k], recv.at[k],
            device_id={"tensor": where}, device_id_type=MESH,
        )

    def to_mid(self, k):
        return self._copy(self.own, self.come, self.s1, self.r1, k, self.inward)

    def swap(self, k):
        return self._copy(self.own, self.total, self.s1, self.r2, k, self.inward)

    def back(self, k):
        return self._copy(self.total, self.total, self.s2, self.r3, k, self.outward)

    def fold(self, k):
        self.to_mid(k).wait_recv()
        at = self.at(k)
        self.own[at, :] = (self.own[at, :].astype(F32) + self.come[at, :].astype(F32)).astype(BF16)
        self.swap(k).start()

    def close(self, k):
        self.swap(k).wait_recv()
        at = self.at(k)
        self.total[at, :] = (self.own[at, :].astype(F32) + self.total[at, :].astype(F32)).astype(BF16)
        self.back(k).start()

    def drain(self, pieces):
        @pl.when(self.mid)
        def _():
            def go(k, c):
                self.swap(k).wait_send()
                self.back(k).wait_send()
                return c

            lax.fori_loop(0, self.li // SUB, go, 0)
            for k in range(self.li // SUB, pieces):
                go(k, 0)

        @pl.when(self.end)
        def _():
            def go(k, c):
                self.to_mid(k).wait_send()
                return c

            lax.fori_loop(0, self.li // SUB, go, 0)
            for k in range(self.li // SUB, pieces):
                go(k, 0)


def z_scratch(rows, pieces):
    return [pltpu.VMEM((rows, D), BF16)] * 2 + [DMA((pieces,))] * 5


def ln_kernel(li, x_ref, mod_ref, o_ref):
    def block(r0, n, s):
        m, _ = norm_rows(x_ref[pl.ds(r0, n), :].astype(F32))
        o_ref[pl.ds(r0, n), :] = (m * (1.0 + mod_ref[6 * s + 1 : 6 * s + 2, :]) + mod_ref[6 * s : 6 * s + 1, :]).astype(BF16)

    def body(i, c):
        block(pl.multiple_of(i * 64, 64), 64, 0)
        return c

    lax.fori_loop(0, li // 64, body, 0)
    block(li, x_ref.shape[0] - li, 1)


def ln_call(x, mod, li):
    return pl.pallas_call(
        functools.partial(ln_kernel, li),
        out_shape=jax.ShapeDtypeStruct(x.shape, BF16),
        in_specs=[VM, VM],
        out_specs=VM,
        compiler_params=pltpu.CompilerParams(vmem_limit_bytes=24 << 20),
    )(x, mod)


def half_lanes(rows, low):
    lane = lax.broadcasted_iota(jnp.int32, rows.shape, 1)
    return jnp.where((lane < HEAD_DIM) == low, rows, jnp.zeros_like(rows))


def qkv_attend_kernel(
    size, li, valid, n_ref, w_ref, b_ref, qkv_ref, o_ref, total, own, come, km, vm, *sems
):
    rows, width = qkv_ref.shape
    cols = width // 3
    z = ZSum(size, li, own, come, total, sems)
    image_pieces = li // SUB
    text = (image_pieces, image_pieces + 1)
    step, per, lag = 256, 256 // SUB, 2
    z.barrier()

    def project(r0, n, s):
        got = dot(n_ref[pl.ds(r0, n), :], w_ref[s, :, :width]) + b_ref[s : s + 1, :]
        qkv_ref[pl.ds(r0, n), :] = got.astype(BF16)

    def project_image(i, c):
        project(pl.multiple_of(i * step, step), step, 0)
        return c

    project(li, rows - li, 1)
    lax.fori_loop(0, li // step, project_image, 0)

    def lanes(j, p):
        return slice(j * cols + p * PAIR, j * cols + (p + 1) * PAIR)

    pairs = cols // PAIR
    for p in range(pairs):
        for h in range(2):
            km[2 * p + h] = half_lanes(qkv_ref[:, lanes(1, p)], h == 0)
            vm[2 * p + h] = half_lanes(qkv_ref[:, lanes(2, p)], h == 0)

    def block(r0, n, s):
        at = pl.ds(r0, n)
        for p in range(pairs):
            q2 = qkv_ref[at, lanes(0, p)]
            mixed = 0.0
            for h in range(2):
                scores = dot(q2, km[2 * p + h], NT)
                col = lax.broadcasted_iota(jnp.int32, scores.shape, 1)
                scores = jnp.where(col < valid, scores, -1e30)
                e = jnp.exp((scores - jnp.max(scores, axis=1, keepdims=True)) * HEAD_DIM**-0.5)
                norm = 1.0 / jnp.sum(e, axis=1, keepdims=True)
                mixed = mixed + dot(e.astype(BF16), vm[2 * p + h]) * norm
            o_ref[at, lanes(0, p)] = mixed.astype(BF16)
        own[at, :] = dot(o_ref[at, :], w_ref[s, :, width:], NT).astype(BF16)

    block(li, rows - li, 1)

    @pl.when(z.end)
    def _():
        for k in text:
            z.to_mid(k).start()

    def image_block(i, c):
        block(pl.multiple_of(i * step, step), step, 0)

        @pl.when(z.end)
        def _():
            for j in range(per):
                z.to_mid(i * per + j).start()

        @pl.when(z.mid & (i == 0))
        def _():
            for k in text:
                z.fold(k)

        @pl.when(z.mid & (i >= 1))
        def _():
            for j in range(per):
                k = (i - 1) * per + j
                z.fold(k)
                if j >= lag:
                    z.close(k - lag)
                else:
                    @pl.when(i == 1)
                    def _():
                        z.close(text[j])

                    @pl.when(i >= 2)
                    def _():
                        z.close(k - lag)

        return c

    lax.fori_loop(0, li // step, image_block, 0)

    @pl.when(z.mid)
    def _():
        for k in range(image_pieces - per, image_pieces):
            z.fold(k)
            z.close(k - lag)
        for k in range(image_pieces - lag, image_pieces):
            z.close(k)

    @pl.when(z.end)
    def _():
        def go(k, c):
            z.back(k).wait_recv()
            return c

        lax.fori_loop(0, image_pieces, go, 0)
        for k in text:
            go(k, 0)

    z.drain(image_pieces + 2)


def qkv_attend_call(normed, weight, bias, size, li, valid, cid):
    rows, width = normed.shape[0], bias.shape[1]
    pieces = li // SUB + 2
    shape = jax.ShapeDtypeStruct
    heads = width // 3 // HEAD_DIM
    return pl.pallas_call(
        functools.partial(qkv_attend_kernel, size, li, valid),
        out_shape=[shape((rows, width), BF16), shape((rows, width // 3), BF16), shape((rows, D), BF16)],
        in_specs=[VM] * 3,
        out_specs=[VM] * 3,
        scratch_shapes=[
            pltpu.VMEM((rows, D), BF16), pltpu.VMEM((rows, D), BF16),
            pltpu.VMEM((heads, rows, PAIR), BF16), pltpu.VMEM((heads, rows, PAIR), BF16),
        ] + [DMA((pieces,))] * 5,
        compiler_params=pltpu.CompilerParams(
            collective_id=cid, has_side_effects=True, vmem_limit_bytes=60 << 20
        ),
    )(normed, weight, bias)


def grads_kernel(li, groups, *refs):
    out = refs[-1]
    at = 0
    for left, right, gate in groups:
        l_ref, r_ref = refs[left], refs[right]
        n = r_ref.shape[1]
        for s in (0, 1):
            span = slice(0, li) if s == 0 else slice(li, l_ref.shape[0])
            lhs = l_ref[span, :]
            if gate is not None:
                g_ref, row = refs[gate[0]], 6 * s + gate[1]
                lhs = (g_ref[row : row + 1, :] * lhs.astype(F32)).astype(BF16)
            got = lax.dot_general(lhs, r_ref[span, :], (((0,), (0,)), ((), ())), preferred_element_type=F32)
            out[:, at : at + n] = got.astype(BF16)
            at += n


def grads_call(pairs, mod, li):
    block = 256
    args, specs, groups = [], [], []
    total = 0
    for left, right, gated in pairs:
        rows = left.shape[0]
        args += [left, right]
        specs += [
            pl.BlockSpec((rows, block), lambda i: (0, i)),
            pl.BlockSpec(right.shape, lambda i: (0, 0), pipeline_mode=pl.Buffered(1)),
        ]
        groups.append((len(args) - 2, len(args) - 1, gated))
        total += 2 * right.shape[1]
    if any(gated for _, _, gated in pairs):
        args.append(mod)
        specs.append(pl.BlockSpec((mod.shape[0], block), lambda i: (0, i)))
    groups = [(l, r, (len(args) - 1, 5) if gated else None) for l, r, gated in groups]
    return pl.pallas_call(
        functools.partial(grads_kernel, li, groups),
        grid=(D // block,),
        out_shape=jax.ShapeDtypeStruct((D, total), BF16),
        in_specs=specs,
        out_specs=pl.BlockSpec((block, total), lambda i: (i, 0)),
        compiler_params=pltpu.CompilerParams(vmem_limit_bytes=60 << 20),
    )(*args)


def proj_sum_kernel(size, li, dims, x_ref, w_ref, total, own, come, *sems):
    rows = x_ref.shape[0]
    z = ZSum(size, li, own, come, total, sems)
    image_pieces = li // SUB
    pieces = image_pieces + 2
    z.barrier()
    step = 256

    def project(r0, n, s):
        own[pl.ds(r0, n), :] = dot(x_ref[pl.ds(r0, n), :], w_ref[s, :, : x_ref.shape[1]], dims).astype(BF16)

    project(li, rows - li, 1)

    @pl.when(z.end)
    def _():
        for k in range(image_pieces, pieces):
            z.to_mid(k).start()

    def image_block(i, c):
        project(pl.multiple_of(i * step, step), step, 0)

        @pl.when(z.end)
        def _():
            for j in range(step // SUB):
                z.to_mid(i * (step // SUB) + j).start()

        return c

    lax.fori_loop(0, li // step, image_block, 0)
    first, second = image_pieces, image_pieces + 1

    @pl.when(z.mid)
    def _():
        lag = 2
        for k in (first, second):
            z.fold(k)
        for k in range(lag):
            z.fold(k)
        z.close(first)
        z.close(second)

        def go(k, c):
            z.fold(k)
            z.close(k - lag)
            return c

        lax.fori_loop(lag, image_pieces, go, 0)
        for k in range(image_pieces - lag, image_pieces):
            z.close(k)

    @pl.when(z.end)
    def _():
        def go(k, c):
            z.back(k).wait_recv()
            return c

        lax.fori_loop(0, image_pieces, go, 0)
        go(first, 0)
        go(second, 0)

    z.drain(pieces)


def proj_sum_call(x, w, size, li, dims, cid):
    rows = x.shape[0]
    pieces = li // SUB + 2
    return pl.pallas_call(
        functools.partial(proj_sum_kernel, size, li, dims),
        out_shape=jax.ShapeDtypeStruct((rows, D), BF16),
        in_specs=[VM] * 2,
        out_specs=VM,
        scratch_shapes=z_scratch(rows, pieces),
        compiler_params=pltpu.CompilerParams(
            collective_id=cid, has_side_effects=True, vmem_limit_bytes=48 << 20
        ),
    )(x, w)


ROOT_2_PI = math.sqrt(2.0 / math.pi)


def gelu_and_slope(x):
    square = x * x
    t = jnp.tanh(ROOT_2_PI * x * (1.0 + 0.044715 * square))
    half = 0.5 * (1.0 + t)
    slope = half + 0.5 * x * (1.0 - t * t) * (ROOT_2_PI * (1.0 + 3 * 0.044715 * square))
    return x * half, slope


def mlp_kernel(
    size, li,
    a_ref, x_hbm, g_hbm, w_hbm, wo_hbm, mod_ref, ob_ref, ib_ref,
    n2_hbm, act_hbm, du_hbm, pm_hbm, dr_hbm, da_hbm, dmix_ref, sums_ref,
    xv, gv, wi, wm, wo_ref, own, come, total, st_n2, st_act, st_du, st_pm, st_dr, st_da, load, put, *sems,
):
    rows = a_ref.shape[0]
    hid, cols = wi.shape[2], wo_ref.shape[2]
    z = ZSum(size, li, own, come, total, sems)
    chunk = 2 * SUB
    chunks = li // chunk
    lt = rows - li
    text = (li // SUB, li // SUB + 1)
    loads = [
        pltpu.make_async_copy(x_hbm, xv, load.at[0]),
        pltpu.make_async_copy(g_hbm, gv, load.at[1]),
        pltpu.make_async_copy(w_hbm.at[1, :, pl.ds(0, hid)], wi.at[1], load.at[2]),
        pltpu.make_async_copy(w_hbm.at[1, :, pl.ds(hid, hid)], wm.at[1], load.at[3]),
        pltpu.make_async_copy(w_hbm.at[0, :, pl.ds(0, hid)], wi.at[0], load.at[4]),
        pltpu.make_async_copy(w_hbm.at[0, :, pl.ds(hid, hid)], wm.at[0], load.at[5]),
        pltpu.make_async_copy(wo_hbm.at[:, :, pl.ds(3 * cols, cols)], wo_ref, load.at[6]),
    ]
    for copy in loads:
        copy.start()
    z.barrier()
    sums_ref[...] = jnp.zeros_like(sums_ref)
    outs = ((st_n2, n2_hbm), (st_act, act_hbm), (st_du, du_hbm), (st_pm, pm_hbm), (st_dr, dr_hbm), (st_da, da_hbm))

    def store(j, r0, n, slot):
        stage, hbm = outs[j]
        return pltpu.make_async_copy(
            stage.at[slot, pl.ds(0, n), :], hbm.at[pl.ds(r0, n), :], put.at[j, slot]
        )

    def resid_of(at, s):
        branch = a_ref[at, :].astype(F32) + ob_ref[s : s + 1, :]
        resid = xv[at, :].astype(F32) + mod_ref[6 * s + 2 : 6 * s + 3, :] * branch
        m, rstd = norm_rows(resid)
        return branch, m, rstd

    def add_sum(s, j, value):
        sums_ref[8 * s + j : 8 * s + j + 1, :] += jnp.sum(value, axis=0, keepdims=True)

    def forward(r0, n, s, slot):
        at = pl.ds(r0, n)
        _, m, _ = resid_of(at, s)
        st_n2[slot, :n, :] = (m * (1.0 + mod_ref[6 * s + 4 : 6 * s + 5, :]) + mod_ref[6 * s + 3 : 6 * s + 4, :]).astype(BF16)
        d_mlp = mod_ref[6 * s + 5 : 6 * s + 6, :] * gv[at, :].astype(F32)
        add_sum(s, 5, d_mlp)
        d_mlp = d_mlp.astype(BF16)
        width = 512
        for j in range(hid // width):
            cols = slice(j * width, (j + 1) * width)
            upper = dot(st_n2[slot, :n, :], wi[s, :, cols]) + ib_ref[s : s + 1, cols]
            act, slope = gelu_and_slope(upper)
            st_act[slot, :n, cols] = act.astype(BF16)
            d_upper = (dot(d_mlp, wm[s, :, cols]) * slope).astype(BF16)
            st_du[slot, :n, cols] = d_upper
            sums_ref[8 * s + 4 : 8 * s + 5, cols] += jnp.sum(d_upper.astype(F32), axis=0, keepdims=True)
        own[at, :] = dot(st_du[slot, :n, :], wi[s], NT).astype(BF16)
        for k in (0, 1, 2):
            store(k, r0, n, slot).start()

    def partial(r0, n, s, slot):
        st_pm[slot, :n, :] = dot(st_act[slot, :n, :], wm[s], NT).astype(BF16)
        store(3, r0, n, slot).start()

    def backward(r0, n, s, slot):
        at = pl.ds(r0, n)
        branch, m, rstd = resid_of(at, s)
        d_mid = total[at, :].astype(F32)
        add_sum(s, 0, d_mid)
        add_sum(s, 1, d_mid * m)
        e = d_mid * (1.0 + mod_ref[6 * s + 4 : 6 * s + 5, :])
        back = (e - jnp.mean(e, axis=-1, keepdims=True) - m * jnp.mean(e * m, axis=-1, keepdims=True)) * rstd
        d_resid = back + gv[at, :].astype(F32)
        st_dr[slot, :n, :] = d_resid
        add_sum(s, 2, d_resid * branch)
        d_attn = mod_ref[6 * s + 2 : 6 * s + 3, :] * d_resid
        add_sum(s, 3, d_attn)
        low = d_attn.astype(BF16)
        st_da[slot, :n, :] = low
        dmix_ref[at, :] = dot(low, wo_ref[s]).astype(BF16)
        for k in (4, 5):
            store(k, r0, n, slot).start()

    for j in (0, 1, 2, 3):
        loads[j].wait()
    forward(li, lt, 1, 2)

    @pl.when(z.end)
    def _():
        for k in text:
            z.to_mid(k).start()

    partial(li, lt, 1, 2)
    for j in (4, 5, 6):
        loads[j].wait()

    def at_chunk(i):
        return pl.multiple_of(i * chunk, chunk)

    def step(i, c):
        slot = lax.rem(i, 2)

        @pl.when((i >= 2) & (i < chunks))
        def _():
            for j in (0, 1, 2, 3):
                store(j, at_chunk(i - 2), chunk, slot).wait()

        @pl.when(i < chunks)
        def _():
            forward(at_chunk(i), chunk, 0, slot)

            @pl.when(z.end)
            def _():
                z.to_mid(2 * i).start()
                z.to_mid(2 * i + 1).start()

            partial(at_chunk(i), chunk, 0, slot)

        @pl.when(z.mid & (i == 0))
        def _():
            for k in text:
                z.fold(k)

        @pl.when(z.mid & (i >= 1) & (i <= chunks))
        def _():
            z.fold(2 * (i - 1))
            z.fold(2 * (i - 1) + 1)

        @pl.when(z.mid & (i == 1))
        def _():
            for k in text:
                z.close(k)

        @pl.when(z.mid & (i >= 2) & (i <= chunks + 1))
        def _():
            z.close(2 * (i - 2))
            z.close(2 * (i - 2) + 1)

        @pl.when(i >= 5)
        def _():
            for j in (4, 5):
                store(j, at_chunk(i - 5), chunk, lax.rem(i - 3, 2)).wait()

        @pl.when(i >= 3)
        def _():
            @pl.when(z.end)
            def _():
                z.back(2 * (i - 3)).wait_recv()
                z.back(2 * (i - 3) + 1).wait_recv()

            backward(at_chunk(i - 3), chunk, 0, lax.rem(i - 3, 2))

        return c

    lax.fori_loop(0, chunks + 3, step, 0)

    @pl.when(z.end)
    def _():
        for k in text:
            z.back(k).wait_recv()

    backward(li, lt, 1, 2)
    for j in range(6):
        store(j, li, lt, 2).wait()
        for i in (chunks - 2, chunks - 1):
            store(j, i * chunk, chunk, i % 2).wait()
    z.drain(len(text) + li // SUB)


def mlp_call(a, x, g, w, wo, mod, ob, ib, cols, size, li, cid):
    rows, hid = a.shape[0], ib.shape[1]
    pieces = li // SUB + 2
    lt = rows - li
    shape = jax.ShapeDtypeStruct
    tall = max(lt, 2 * SUB)
    return pl.pallas_call(
        functools.partial(mlp_kernel, size, li),
        out_shape=[
            shape((rows, D), BF16), shape((rows, hid), BF16), shape((rows, hid), BF16), shape((rows, D), BF16),
            shape((rows, D), F32), shape((rows, D), BF16), shape((rows, cols), BF16), shape((16, D), F32),
        ],
        in_specs=[VM, ANY, ANY, ANY, ANY, VM, VM, VM],
        out_specs=[ANY] * 6 + [VM] * 2,
        scratch_shapes=[
            pltpu.VMEM((rows, D), BF16), pltpu.VMEM((rows, D), BF16),
            pltpu.VMEM((2, D, hid), BF16), pltpu.VMEM((2, D, hid), BF16), pltpu.VMEM((2, D, cols), BF16),
            pltpu.VMEM((rows, D), BF16), pltpu.VMEM((rows, D), BF16), pltpu.VMEM((rows, D), BF16),
            pltpu.VMEM((3, tall, D), BF16), pltpu.VMEM((3, tall, hid), BF16), pltpu.VMEM((3, tall, hid), BF16),
            pltpu.VMEM((3, tall, D), BF16), pltpu.VMEM((3, tall, D), F32), pltpu.VMEM((3, tall, D), BF16),
            DMA((7,)), DMA((6, 3)),
        ] + [DMA((pieces,))] * 5,
        compiler_params=pltpu.CompilerParams(
            collective_id=cid, has_side_effects=True, vmem_limit_bytes=VMEM_MAX
        ),
    )(a, x, g, w, wo, mod, ob, ib)


def attend_back_kernel(
    size, li, valid, qkv_ref, do_ref, pm_hbm, d_ref, total, own, come, dk_acc, dv_acc, kt, load, *sems
):
    rows, width = qkv_ref.shape
    cols = width // 3
    z = ZSum(size, li, own, come, total, sems)
    image_pieces = li // SUB
    text = (image_pieces, image_pieces + 1)
    fetch = pltpu.make_async_copy(pm_hbm, own, load)
    fetch.start()
    z.barrier()
    fetch.wait()

    @pl.when(z.end)
    def _():
        for k in text:
            z.to_mid(k).start()

        def go(k, c):
            z.to_mid(k).start()
            return c

        lax.fori_loop(0, image_pieces, go, 0)

    lag = 2
    per_pair = li // 256

    def tick(k):
        @pl.when(z.mid & (k < image_pieces))
        def _():
            z.fold(k)

        @pl.when(z.mid & (k >= lag) & (k < image_pieces + lag))
        def _():
            z.close(k - lag)

    for p in range(cols // PAIR):
        at = lambda j: slice(j * cols + p * PAIR, j * cols + (p + 1) * PAIR)
        k2, v2 = qkv_ref[:, at(1)], qkv_ref[:, at(2)]
        kt[...] = k2.astype(F32).T.astype(BF16)
        ks = [half_lanes(k2, low) for low in (True, False)]
        vs = [half_lanes(v2, low) for low in (True, False)]
        dk_acc[...] = jnp.zeros_like(dk_acc)
        dv_acc[...] = jnp.zeros_like(dv_acc)

        def block(r0, n):
            q2 = qkv_ref[pl.ds(r0, n), at(0)]
            g2 = do_ref[pl.ds(r0, n), at(0)]
            parts = []
            for h in range(2):
                s = dot(ks[h], q2, NT)
                row = lax.broadcasted_iota(jnp.int32, s.shape, 0)
                s = jnp.where(row < valid, s, -1e30)
                e = jnp.exp((s - jnp.max(s, axis=0, keepdims=True)) * HEAD_DIM**-0.5)
                probs = e * (1.0 / jnp.sum(e, axis=0, keepdims=True))
                d_probs = dot(vs[h], g2, NT)
                delta = jnp.sum(probs * d_probs, axis=0, keepdims=True)
                ds = (probs * (d_probs - delta)).astype(BF16)
                dk_acc[...] += dot(ds, half_lanes(q2, h == 0))
                dv_acc[...] += dot(probs.astype(BF16), half_lanes(g2, h == 0))
                parts.append(dot(kt[h * HEAD_DIM : (h + 1) * HEAD_DIM, :], ds))
            d_q = jnp.concatenate(parts, axis=0).T * HEAD_DIM**-0.5
            d_ref[pl.ds(r0, n), at(0)] = d_q.astype(BF16)

        if p == 0:
            block(li, rows - li)

            @pl.when(z.mid)
            def _():
                for k in text:
                    z.fold(k)

        def image_block(i, c):
            block(pl.multiple_of(i * 256, 256), 256)
            tick(p * (per_pair + 1) + i)
            return c

        lax.fori_loop(0, per_pair, image_block, 0)
        if p == 0:
            @pl.when(z.mid)
            def _():
                for k in text:
                    z.close(k)
        else:
            block(li, rows - li)
        at_end = p * (per_pair + 1) + per_pair

        @pl.when(z.mid)
        def _():
            z.fold(at_end)
            z.close(at_end - lag)

        d_ref[:, at(1)] = (dk_acc[...] * HEAD_DIM**-0.5).astype(BF16)
        d_ref[:, at(2)] = dv_acc[...].astype(BF16)

    def rest(k, c):
        tick(k)
        return c

    lax.fori_loop((cols // PAIR) * (per_pair + 1), image_pieces + lag, rest, 0)

    @pl.when(z.end)
    def _():
        def go(k, c):
            z.back(k).wait_recv()
            return c

        lax.fori_loop(0, image_pieces, go, 0)
        for k in text:
            go(k, 0)

    z.drain(image_pieces + 2)


def attend_back_call(qkv, d_mix, pm, size, li, valid, cid):
    rows, width = qkv.shape
    pieces = li // SUB + 2
    return pl.pallas_call(
        functools.partial(attend_back_kernel, size, li, valid),
        out_shape=[jax.ShapeDtypeStruct((rows, width), BF16), jax.ShapeDtypeStruct((rows, D), BF16)],
        in_specs=[VM, VM, ANY],
        out_specs=[VM, VM],
        scratch_shapes=[
            pltpu.VMEM((rows, D), BF16), pltpu.VMEM((rows, D), BF16),
            pltpu.VMEM((rows, PAIR), F32), pltpu.VMEM((rows, PAIR), F32), pltpu.VMEM((PAIR, rows), BF16), DMA,
        ] + [DMA((pieces,))] * 5,
        compiler_params=pltpu.CompilerParams(
            collective_id=cid, has_side_effects=True, vmem_limit_bytes=60 << 20
        ),
    )(qkv, d_mix, pm)


def shards(
    image, text, pooled, timestep, grad_image, grad_text, ada_weight, ada_bias, qkv_weight, qv_bias,
    out_weight, out_bias, mlp_in_weight, mlp_in_bias, mlp_out_weight, mlp_out_bias,
):
    size = lax.axis_size("tensor")
    li, lt = image.shape[1], text.shape[1]
    pad = -lt % 16
    spans = (slice(0, li), slice(li, li + lt + pad))
    valid = li + lt
    cols = out_weight.shape[1]

    def joint(image_rows, text_rows):
        return jnp.concatenate([image_rows[0], jnp.pad(text_rows[0], ((0, pad), (0, 0)))])

    def gather(weight):
        return lax.all_gather(weight, "dp", axis=1, tiled=True)

    x, g = joint(image, text), joint(grad_image, grad_text)
    packed = jnp.concatenate(
        [qkv_weight.reshape(2, qkv_weight.shape[1], -1), jnp.swapaxes(out_weight, 1, 2)], axis=2
    )
    packed, pooled = lax.optimization_barrier((packed, pooled))
    w_attn = gather(packed)
    w_mlp = gather(jnp.concatenate([mlp_in_weight, jnp.swapaxes(mlp_out_weight, 1, 2)], axis=2))

    width_local = pooled.shape[1]
    first_col = lax.axis_index("tensor") * width_local
    condition = pooled.astype(F32) + time_embed(timestep, first_col, width_local)
    cond_act, silu_pull = jax.vjp(jax.nn.silu, condition)
    cond_all = lax.all_gather(cond_act.astype(BF16), "dp", axis=0, tiled=True)
    mod_part = jnp.einsum("sc,nce->nse", cond_all, ada_weight, preferred_element_type=F32)
    mod_part = lax.all_to_all(mod_part, "dp", split_axis=1, concat_axis=2, tiled=True)
    modul = lax.psum(mod_part, "tensor") + ada_bias.astype(F32)[:, None, :]
    mod = modul.reshape(12, D)

    out_b, in_b, last_b = out_bias.astype(F32), mlp_in_bias.astype(F32), mlp_out_bias.astype(F32)
    qkv_b = jnp.stack([qv_bias[:, 0], jnp.zeros_like(qv_bias[:, 0]), qv_bias[:, 1]], axis=1)
    qkv_b = qkv_b.reshape(2, -1).astype(F32)

    normed = ln_call(x, mod, li)
    qkv, mixed, attn = qkv_attend_call(normed, w_attn, qkv_b, size, li, valid, 1)
    normed2, act, d_upper, mlp_part, d_resid, d_attn, d_mix, sums = mlp_call(
        attn, x, g, w_mlp, w_attn, mod, out_b, in_b, cols, size, li, 2
    )

    def scatter(grad):
        return lax.psum_scatter(grad, "dp", scatter_dimension=0, tiled=True).astype(F32)

    hid = mlp_in_bias.shape[1]
    mlp_grads = grads_call([(normed2, d_upper, False), (g, act, True)], mod, li)
    mlp_grads, mlp_part = lax.optimization_barrier((mlp_grads, mlp_part))
    mlp_shard = scatter(mlp_grads)
    w_in_grad = jnp.stack([mlp_shard[:, :hid], mlp_shard[:, hid : 2 * hid]])
    w_mlp_grad = jnp.stack([mlp_shard[:, 2 * hid : 3 * hid].T, mlp_shard[:, 3 * hid :].T])

    d_qkv, mlp = attend_back_call(qkv, d_mix, mlp_part, size, li, valid, 3)
    attn_grads = grads_call([(d_attn, mixed, False), (normed, d_qkv, False)], mod, li)
    attn_grads, d_qkv = lax.optimization_barrier((attn_grads, d_qkv))
    attn_shard = scatter(attn_grads)
    w_out_grad = jnp.stack([attn_shard[:, :cols].T, attn_shard[:, cols : 2 * cols].T])
    qkv_grad = jnp.stack([attn_shard[:, 2 * cols : 5 * cols], attn_shard[:, 5 * cols :]])
    d_in = proj_sum_call(d_qkv, w_attn, size, li, NT, 4)

    blocks, token_grads, d_mods = [], [], []
    for s in (0, 1):
        rows = slice(0, li) if s == 0 else slice(li, li + lt)
        xs, gs = x[rows].astype(F32), g[rows].astype(F32)
        second = mlp[rows].astype(F32) + last_b[s]
        resid = xs + mod[6 * s + 2] * (attn[rows].astype(F32) + out_b[s])
        blocks.append((resid + mod[6 * s + 5] * second).astype(BF16)[None])
        d_gate2 = jnp.sum(gs * second, axis=0)
        m, rstd = norm_rows(xs)
        d = d_in[rows].astype(F32)
        d_shift, d_scale = jnp.sum(d, axis=0), jnp.sum(d * m, axis=0)
        e = d * (1.0 + mod[6 * s + 1])
        back = (e - jnp.mean(e, axis=-1, keepdims=True) - m * jnp.mean(e * m, axis=-1, keepdims=True)) * rstd
        token_grads.append((d_resid[rows] + back)[None])
        d_mods += [d_shift, d_scale, sums[8 * s + 2], sums[8 * s], sums[8 * s + 1], d_gate2]
    pair = [jnp.sum(d_qkv[spans[s], j * cols : (j + 1) * cols].astype(F32), axis=0) for s in (0, 1) for j in (0, 2)]

    small = d_mods + pair + [sums[8 * s + 3] for s in (0, 1)] + [sums[8 * s + 4] for s in (0, 1)] + [sums[8 * s + 5] for s in (0, 1)]
    every = lax.all_gather(jnp.concatenate(small).astype(BF16), "dp")
    summed = jnp.sum(every.astype(F32), axis=0)
    at = [0]
    for width in (12 * D, 4 * cols, 2 * D, 2 * hid, 2 * D):
        at.append(at[-1] + width)
    pieces = [summed[a:b] for a, b in zip(at, at[1:])]
    ada_cols = ada_weight.shape[2]
    d_mod_cols = lax.dynamic_slice_in_dim(
        every[:, : at[1]].reshape(-1, 2, 6 * D), lax.axis_index("dp") * ada_cols, ada_cols, axis=2
    )
    ada_grad = jnp.einsum("sc,sne->nce", cond_all, d_mod_cols, preferred_element_type=F32)
    d_cond_act = lax.psum_scatter(
        jnp.einsum("sne,nce->sc", d_mod_cols, ada_weight, preferred_element_type=F32),
        "dp", scatter_dimension=0, tiled=True,
    )
    (pooled_grad,) = silu_pull(d_cond_act)
    return (
        blocks[0],
        blocks[1],
        token_grads[0],
        token_grads[1],
        pooled_grad,
        ada_grad,
        pieces[0].reshape(2, 6 * D),
        qkv_grad.reshape(2, -1, 3, cols),
        pieces[1].reshape(2, 2, cols),
        w_out_grad,
        pieces[2].reshape(2, D),
        w_in_grad,
        pieces[3].reshape(2, hid),
        w_mlp_grad,
        pieces[4].reshape(2, D),
    )


def solution(mesh):
    t = "tensor"
    rows, last, mid = P("dp", None, None), P(None, t, "dp"), P(None, "dp", t)
    return jax.shard_map(
        shards,
        mesh=mesh,
        in_specs=(
            rows, rows, P("dp", t), P("dp"), rows, rows, last, P(), P(None, "dp", None, t), P(None, None, t),
            last, P(), mid, P(None, t), last, P(),
        ),
        out_specs=(
            rows, rows, rows, rows, P("dp", t), last, P(), P(None, "dp", None, t), P(None, None, t),
            last, P(), mid, P(None, t), last, P(),
        ),
        check_vma=False,
    )
```
